32 devices in a mesh: band: 4 (over y, x), ga: 8 (over z, core).
Axes of the slice: x: 2, y: 2, z: 4, core: 2. Of those that a mesh axis runs over, the one named last changes fastest.
Arguments:
- psi: float32 [4096, 4096], P('band', 'ga'), may hold values from -6 to 6
- lower: float32 [4096, 4096], P('band', 'ga'), as said below
Outputs:
- orthonormal: float32 [4096, 4096], P('band', 'ga')
- block_intersection: float32 [4096, 1024], P('band')
The draws below stay inside these ranges and needn't reach their ends.
Inputs may be any that keep to these rules, and one draw needn't show every extreme that they name: lower is lower triangular with its diagonal between 1 and 2.
All inputs are finite; a program needn't handle non-finite values.
Results may differ from the reference program's by a relative error of at most 0.00022.
Values sent between devices are 32-bit elements; how exact they have to be, the bound alone decides.
No kernel may reach another device: no remote copies, remote signals or barrier semaphores. Data moves between devices by JAX's collectives and lax.ppermute only.
A program may use at most 64 MiB of HBM per device.

```python
import math
import jax
import jax.numpy as jnp
from jax import lax

NB = 4096
NG = 4096
N_BAND = 4


def draw_lower(key, part):
    first, second = jax.random.split(jax.random.fold_in(key, 11))
    spread = jax.random.normal(first, (NB, NB), jnp.float32) * (2.0 / math.sqrt(NB))
    middle = jax.random.uniform(second, (NB,), jnp.float32, 1.0, 2.0)
    rowpos = lax.broadcasted_iota(jnp.int32, (NB, NB), 0)
    colpos = lax.broadcasted_iota(jnp.int32, (NB, NB), 1)
    return jnp.where(rowpos > colpos, spread, 0.0) + jnp.diag(middle)


def shard_levels(stream_key, extent, pieces, smallest, largest):
    def one(dim, shards_of):
        heights = jax.random.uniform(jax.random.fold_in(jax.random.fold_in(stream_key, 6), dim), (shards_of,), jnp.float32, smallest / len(pieces), largest / len(pieces))
        return jnp.repeat(jnp.exp(heights), extent[dim] // shards_of).reshape((-1,) + (1,) * (len(extent) - dim - 1))

    level = one(*pieces[0])
    for cut in pieces[1:]:
        level = level * one(*cut)
    return level


def bell_draw(key, extent, deviation, bound, shards=(), kind=jnp.bfloat16):
    array = deviation * jax.random.normal(key, extent, jnp.float32)
    if shards:
        array = array * shard_levels(key, extent, shards, -0.22, 0.18)
    return jnp.clip(array, -bound, bound).astype(kind)


def setup_inputs(seed: int = 0) -> dict:
    splits = jax.random.split(jax.random.key(seed), 3)
    psi = bell_draw(splits[0], (NB, NG), 1.0, 6.0, ((0, 4), (1, 8)), jnp.float32)
    lower = draw_lower(jax.random.fold_in(splits[2], 71), 0)
    return {"psi": psi, "lower": lower}


def reference(psi, lower):
    solved = jax.scipy.linalg.solve_triangular(lower, psi, lower=True)
    blocks = solved.reshape(N_BAND, NB // N_BAND, NG)
    intersection = jnp.einsum('bik,bjk->bij', blocks, blocks, precision=lax.Precision.HIGHEST) / NG
    return (solved, intersection.reshape(NB, NB // N_BAND))
```

```python
import functools
import jax
import jax.numpy as jnp
from jax import lax
from jax.experimental import pallas as pl
from jax.experimental.pallas import tpu as pltpu
from jax.sharding import PartitionSpec as P

AXES = ("band", "ga")
F32, BF16 = jnp.float32, jnp.bfloat16
ROWCHUNKS = 2
COLCHUNKS = 2
SUB = 256
TILE = 128


def split(x):
    hi = x.astype(BF16)
    return hi, (x - hi.astype(F32)).astype(BF16)


def mm(a, b, dims=(((1,), (0,)), ((), ()))):
    ah, al = a
    bh, bl = b
    dot = functools.partial(lax.dot_general, dimension_numbers=dims, preferred_element_type=F32)
    return dot(ah, bh) + (dot(ah, bl) + dot(al, bh))


def load_block(cands, lbuf, sem, own_chip, core, half):
    for wait in (False, True):
        for chip, (mine, other) in enumerate(cands):
            for side in range(2):
                for pieces, col in ((mine, side), (other, 1 - side)):
                    row = 0
                    for piece in pieces:
                        take = piece.shape[0]
                        copy = pltpu.make_async_copy(
                            piece, lbuf.at[pl.ds(row, take), pl.ds(col * half, half)], sem
                        )
                        row += take

                        @pl.when((own_chip == chip) & (core == side))
                        def _():
                            if wait:
                                copy.wait()
                            else:
                                copy.start()


def unflatten(refs, nq, pieces):
    it = iter(refs)
    return [
        ([next(it) for _ in range(pieces)], [next(it) for _ in range(pieces)]) for _ in range(nq)
    ]


def flatten(cands):
    return [piece for mine, other in cands for piece in mine + other]


def update_kernel(s, nq, pieces, *refs):
    nc = nq * 2 * pieces
    r_ref, y_ref = refs[0], refs[1]
    cands = unflatten(refs[2 : 2 + nc], nq, pieces)
    o_ref, lbuf, sem = refs[2 + nc :]
    band, ga = lax.axis_index("band"), lax.axis_index("ga")
    n = lbuf.shape[0]

    @pl.when(band > s)
    def _():
        load_block(cands, lbuf, sem, ga // 2, ga % 2, n // 2)
        y = split(y_ref[...])
        for i in range(n // SUB):
            rows = pl.ds(i * SUB, SUB)
            o_ref[rows, :] = r_ref[rows, :] - mm(split(lbuf[rows, :]), y)

    @pl.when(band <= s)
    def _():
        o_ref[...] = r_ref[...]


def invert_kernel(s, nq, pieces, *refs):
    nc = nq * 2 * pieces
    cands = unflatten(refs[:nc], nq, pieces)
    o_ref, lbuf, sem = refs[nc:]
    band, ga = lax.axis_index("band"), lax.axis_index("ga")
    n = lbuf.shape[0]

    @pl.when(band == s)
    def _():
        load_block(cands, lbuf, sem, ga // 2, ga % 2, n // 2)
        row = lax.broadcasted_iota(jnp.int32, (SUB, SUB), 0)
        col = lax.broadcasted_iota(jnp.int32, (SUB, SUB), 1)
        count = n // SUB
        tiles = [lbuf[pl.ds(i * SUB, SUB), pl.ds(i * SUB, SUB)] for i in range(count)]
        inv = []
        for t in tiles:
            d = jnp.where(row == col, t, 0.0)
            rd = 1.0 / jnp.sum(d, axis=1, keepdims=True)
            cd = 1.0 / jnp.sum(d, axis=0, keepdims=True)
            pair = (row == col + 1) & (row % 2 == 1)
            inv.append(jnp.where(row == col, rd, jnp.where(pair, -t * rd * cd, 0.0)))
        m = 2
        while m < SUB:
            mask = (row // (2 * m) == col // (2 * m)) & ((row // m) % 2 == 1) & ((col // m) % 2 == 0)
            xs = [split(x) for x in inv]
            cs = [split(jnp.where(mask, t, 0.0)) for t in tiles]
            mid = [mm(c, x) for c, x in zip(cs, xs)]
            inv = [x - mm(xx, split(v)) for x, xx, v in zip(inv, xs, mid)]
            m *= 2
        for i, x in enumerate(inv):
            o_ref[pl.ds(i * SUB, SUB), :] = x


def solve_kernel(s, nq, pieces, *refs):
    nc = nq * 2 * pieces
    r_ref, i_ref = refs[0], refs[1]
    cands = unflatten(refs[2 : 2 + nc], nq, pieces)
    o_ref, lbuf, sem = refs[2 + nc :]
    band, ga = lax.axis_index("band"), lax.axis_index("ga")
    n = lbuf.shape[0]

    @pl.when(band == s)
    def _():
        load_block(cands, lbuf, sem, ga // 2, ga % 2, n // 2)
        o_ref[...] = r_ref[...]
        for i in range(n // SUB):
            rows = pl.ds(i * SUB, SUB)
            y = mm(split(i_ref[rows, :]), split(o_ref[rows, :]))
            o_ref[rows, :] = y
            rest = n - (i + 1) * SUB
            if rest:
                below = pl.ds((i + 1) * SUB, rest)
                o_ref[below, :] = o_ref[below, :] - mm(split(lbuf[below, rows]), split(y))

    @pl.when(band != s)
    def _():
        o_ref[...] = r_ref[...]


def cost(flops, data):
    return pl.CostEstimate(flops=flops, bytes_accessed=data, transcendentals=0)


VM = pl.BlockSpec(memory_space=pltpu.VMEM)
ANY = pl.BlockSpec(memory_space=pl.ANY)


def call(kernel, vmem_args, cands, out_shape, n, flops):
    flat = flatten(cands)
    pieces = len(cands[0][0])
    return pl.pallas_call(
        functools.partial(kernel, len(cands), pieces),
        out_shape=jax.ShapeDtypeStruct(out_shape, F32),
        in_specs=[VM] * len(vmem_args) + [ANY] * len(flat),
        out_specs=VM,
        scratch_shapes=[pltpu.VMEM((n, n), F32), pltpu.SemaphoreType.DMA],
        compiler_params=pltpu.CompilerParams(vmem_limit_bytes=48 * 2**20),
        cost_estimate=cost(flops, 4 * n * n),
    )(*vmem_args, *flat)


def gram_kernel(y_ref, o_ref):
    n = y_ref.shape[0]
    y = split(y_ref[...])
    row = 0
    for i in range(n // TILE):
        part = tuple(v[i * TILE : (i + 1) * TILE] for v in y)
        upto = tuple(v[: (i + 1) * TILE] for v in y)
        g = mm(upto, part, (((1,), (1,)), ((), ())))
        o_ref[pl.ds(row, (i + 1) * TILE), :] = g
        row += (i + 1) * TILE


def unpack_kernel(scale, p_ref, o_ref):
    n = o_ref.shape[0]
    row = 0
    for i in range(n // TILE):
        here = pl.ds(i * TILE, TILE)
        for j in range(i + 1):
            block = p_ref[pl.ds(row, TILE), :] * scale
            row += TILE
            o_ref[pl.ds(j * TILE, TILE), here] = block
            if j < i:
                o_ref[here, pl.ds(j * TILE, TILE)] = block.T


def plain(kernel, out_shape, flops, *args):
    return pl.pallas_call(
        kernel,
        out_shape=jax.ShapeDtypeStruct(out_shape, F32),
        in_specs=[VM] * len(args),
        out_specs=VM,
        compiler_params=pltpu.CompilerParams(vmem_limit_bytes=48 * 2**20),
        cost_estimate=cost(flops, 4 * out_shape[0] * out_shape[1]),
    )(*args)


def local(psi, lower):
    nb, ng = lax.axis_size("band"), lax.axis_size("ga")
    nq = ng // 2
    n, w = psi.shape
    ga = lax.axis_index("ga")
    chip, core = ga // 2, ga % 2

    def shift(x, rule):
        pairs = []
        for b in range(nb):
            for q in range(nq):
                for c in range(2):
                    to = rule(b, q, c)
                    if to is not None:
                        pairs.append((b * ng + q * 2 + c, to[0] * ng + to[1] * 2 + to[2]))
        return lax.ppermute(x, AXES, pairs)

    def swap(x, keep):
        return shift(x, lambda b, q, c: (b, q, 1 - c) if keep(b, q) else None)

    rows = n // ROWCHUNKS
    own = [lower[i * rows : (i + 1) * rows] for i in range(ROWCHUNKS)]
    table = [[None] * nq for _ in range(nb)]
    own_other = [swap(x, lambda b, q: b >= q) for x in own]
    fromleft, fromright = {}, {}
    left, right = own, own
    for t in range(1, nq):
        left = [
            shift(x, lambda b, q, c: (b, q + 1, c) if q + 1 < nq and 0 <= q - t + 1 <= b else None)
            for x in left
        ]
        right = [
            shift(x, lambda b, q, c: (b, q - 1, c) if q >= 1 and q + t - 1 <= min(b, nq - 1) else None)
            for x in right
        ]
        fromleft[t] = (left, [swap(x, lambda b, q: 0 <= q - t <= b) for x in left])
        fromright[t] = (right, [swap(x, lambda b, q: q + t <= min(b, nq - 1)) for x in right])
    for s in range(nb):
        for q in range(nq):
            if q == s:
                table[s][q] = (own, own_other)
            elif q > s:
                table[s][q] = fromleft[q - s]
            else:
                table[s][q] = fromright[s - q]

    wc = w // COLCHUNKS
    rhs = [psi[:, k * wc : (k + 1) * wc] for k in range(COLCHUNKS)]
    for s in range(nb):
        inverse = call(
            functools.partial(invert_kernel, s), [], table[s], (n, SUB), n, 40 * n * SUB * SUB
        )
        for k in range(COLCHUNKS):
            solved = call(
                functools.partial(solve_kernel, s),
                [rhs[k], inverse],
                table[s],
                (n, wc),
                n,
                4 * n * n * wc,
            )
            rhs[k] = solved
            if s == nb - 1:
                continue
            got = {}
            for b in range(s + 1, nb):
                diff = s ^ b
                low = diff & -diff
                if diff != low and (s & diff) == 0 and (b ^ low) in got:
                    src, val = b ^ low, got[b ^ low]
                else:
                    src, val = s, solved
                got[b] = shift(val, lambda bb, q, c: (b, q, c) if bb == src else None)
            total = sum(got.values())
            rhs[k] = call(
                functools.partial(update_kernel, s),
                [solved, total],
                table[s],
                (n, wc),
                n,
                6 * n * n * wc,
            )
    full = jnp.concatenate(rhs, axis=1)

    tri = n // TILE * (n // TILE + 1) // 2 * TILE
    packed = plain(gram_kernel, (tri, TILE), 6 * n * n * w, full)
    every = lambda b, q: True
    half = tri // 2
    mine = lax.dynamic_slice_in_dim(packed, core * half, half, 0)
    give = lax.dynamic_slice_in_dim(packed, (1 - core) * half, half, 0)
    mine = mine + swap(give, every)
    part = half // nq
    piece = lambda q: lax.dynamic_slice_in_dim(mine, q * part, part, 0)
    total = piece(chip)
    for d in range(1, nq):
        total = total + shift(piece(chip ^ d), lambda b, q, c: (b, q ^ d, c))
    result = jnp.zeros((half, TILE), F32)
    result = lax.dynamic_update_slice_in_dim(result, total, chip * part, 0)
    for d in range(1, nq):
        got = shift(total, lambda b, q, c: (b, q ^ d, c))
        result = lax.dynamic_update_slice_in_dim(result, got, (chip ^ d) * part, 0)
    theirs = swap(result, every)
    whole = jnp.zeros((tri, TILE), F32)
    whole = lax.dynamic_update_slice_in_dim(whole, result, core * half, 0)
    whole = lax.dynamic_update_slice_in_dim(whole, theirs, (1 - core) * half, 0)
    inter = plain(functools.partial(unpack_kernel, 1.0 / (w * ng)), (n, n), 4 * n * n, whole)
    return (full, inter)


def solution(mesh):
    return jax.shard_map(
        local,
        mesh=mesh,
        in_specs=(P("band", "ga"), P("band", "ga")),
        out_specs=(P("band", "ga"), P("band", None)),
        check_vma=False,
    )
```

```python
import functools
import jax
import jax.numpy as jnp
from jax import lax
from jax.experimental import pallas as pl
from jax.experimental.pallas import tpu as pltpu
from jax.sharding import PartitionSpec as P

AXES = ("band", "ga")
F32, BF16 = jnp.float32, jnp.bfloat16
PIECES = 2
CHUNKS = 2
SUB = 256
HELPED = {4: {2: (2, 0)}}


def split(x):
    hi = x.astype(BF16)
    return hi, (x - hi.astype(F32)).astype(BF16)


def mm(a, b, dims=(((1,), (0,)), ((), ()))):
    dot = functools.partial(lax.dot_general, dimension_numbers=dims, preferred_element_type=F32)
    return dot(a[0], b[0]) + (dot(a[0], b[1]) + dot(a[1], b[0]))


def tile(i):
    return pl.ds(pl.multiple_of(i * SUB, SUB), SUB)


def loop(count, body):
    lax.fori_loop(0, count, lambda i, _: (body(i), 0)[1], 0)


def invert_kernel(l_ref, o_ref):
    band, ga = lax.axis_index("band"), lax.axis_index("ga")
    n, wide = l_ref.shape
    o_ref[...] = l_ref[...]

    @pl.when(ga // 2 == band)
    def _():
        first = (ga % 2) * wide
        row = lax.broadcasted_iota(jnp.int32, (SUB, SUB), 0)
        col = lax.broadcasted_iota(jnp.int32, (SUB, SUB), 1)
        spots = [
            (pl.ds(pl.multiple_of(first + i * SUB, SUB), SUB), pl.ds(i * SUB, SUB))
            for i in range(wide // SUB)
        ]
        for at in spots:
            t = l_ref[at]
            d = jnp.where(row == col, t, 0.0)
            rd = 1.0 / jnp.sum(d, axis=1, keepdims=True)
            cd = 1.0 / jnp.sum(d, axis=0, keepdims=True)
            pair = (row == col + 1) & (row % 2 == 1)
            o_ref[at] = jnp.where(row == col, rd, jnp.where(pair, -t * rd * cd, 0.0))

        def level(k):
            r, c = lax.shift_right_logical(row, k), lax.shift_right_logical(col, k)
            mask = (r == c + 1) & (r % 2 == 1)
            xs = [o_ref[at] for at in spots]
            ys = [split(x) for x in xs]
            mid = [mm(split(jnp.where(mask, l_ref[at], 0.0)), y) for at, y in zip(spots, ys)]
            for at, x, y, v in zip(spots, xs, ys, mid):
                o_ref[at] = x - mm(y, split(v))

        loop(SUB.bit_length() - 2, lambda k: level(k + 1))


def fetch(blocks, lbuf, sem, core):
    wide = lbuf.shape[2] // 2
    copies = []
    for d, (mine, other) in enumerate(blocks):
        for pieces, side in ((mine, core), (other, 1 - core)):
            row = 0
            for piece in pieces:
                to = lbuf.at[d, pl.ds(row, piece.shape[0]), pl.ds(pl.multiple_of(side * wide, wide), wide)]
                copies.append(pltpu.make_async_copy(piece, to, sem.at[d]))
                row += piece.shape[0]
    return copies


def unflatten(refs, pieces):
    it = iter(refs)
    blocks = []
    while len(blocks) * 2 * pieces < len(refs):
        blocks.append(([next(it) for _ in range(pieces)], [next(it) for _ in range(pieces)]))
    return blocks


def product_update(o_ref, lbuf, d, yh, yl, k):
    n = lbuf.shape[1]
    depth = min(2 * SUB, n)

    def body(t):
        i, j = t // (n // depth), t % (n // depth)
        cols = pl.ds(pl.multiple_of(j * depth, depth), depth)
        part = mm(split(lbuf[d, tile(i), cols]), (yh[k, cols, :], yl[k, cols, :]))
        o_ref[tile(i), :] = o_ref[tile(i), :] - part

    loop(n // SUB * (n // depth), body)


def solve_kernel(s, partial, pieces, *refs):
    given = s - (1 if partial else 0)
    psi_ref = refs[0]
    part_ref = refs[1] if partial else None
    refs = refs[2 if partial else 1 :]
    y_refs, refs = refs[:given], refs[given:]
    count = (given + 1) * 2 * pieces
    blocks = unflatten(refs[:count], pieces)
    o_ref, lbuf, yh, yl, sem = refs[count:]
    band, core = lax.axis_index("band"), lax.axis_index("ga") % 2
    n = lbuf.shape[1]

    @pl.when(band == s)
    def _():
        copies = fetch(blocks, lbuf, sem, core)
        for copy in copies:
            copy.start()
        o_ref[...] = psi_ref[...]
        if partial:
            o_ref[...] = o_ref[...] - part_ref[...]
        for k in range(given):

            def spread(i):
                yh[k, tile(i), :], yl[k, tile(i), :] = split(y_refs[k][tile(i), :])

            loop(n // SUB, spread)
        for copy in copies:
            copy.wait()
        if given:
            loop(given, lambda k: product_update(o_ref, lbuf, k + 1, yh, yl, k))

        def step(i):
            y = mm(split(lbuf[0, tile(i), tile(i)]), split(o_ref[tile(i), :]))
            o_ref[tile(i), :] = y
            y = split(y)

            def below(j, _):
                o_ref[tile(j), :] = o_ref[tile(j), :] - mm(split(lbuf[0, tile(j), tile(i)]), y)
                return 0

            lax.fori_loop(i + 1, n // SUB, below, 0)

        loop(n // SUB, step)


def term_kernel(helper, pieces, y_ref, *refs):
    blocks = unflatten(refs[: 2 * pieces], pieces)
    o_ref, lbuf, yh, yl, sem = refs[2 * pieces :]
    band, core = lax.axis_index("band"), lax.axis_index("ga") % 2
    n = lbuf.shape[1]

    @pl.when(band == helper)
    def _():
        copies = fetch(blocks, lbuf, sem, core)
        for copy in copies:
            copy.start()
        o_ref[...] = jnp.zeros_like(o_ref)

        def spread(i):
            yh[0, tile(i), :], yl[0, tile(i), :] = split(-y_ref[tile(i), :])

        loop(n // SUB, spread)
        for copy in copies:
            copy.wait()
        product_update(o_ref, lbuf, 0, yh, yl, 0)

    @pl.when(band != helper)
    def _():
        o_ref[...] = y_ref[...]


def corner(t, count):
    i = sum((t >= k * (k + 1) // 2).astype(jnp.int32) for k in range(1, count))
    return i, t - i * (i + 1) // 2


def gram_kernel(y_ref, o_ref, yh, yl):
    n = y_ref.shape[0]

    def spread(i):
        yh[tile(i), :], yl[tile(i), :] = split(y_ref[tile(i), :])

    loop(n // SUB, spread)
    count = n // SUB

    def body(t):
        i, j = corner(t, count)
        a, b = (yh[tile(i), :], yl[tile(i), :]), (yh[tile(j), :], yl[tile(j), :])
        o_ref[tile(t), :] = mm(a, b, (((1,), (1,)), ((), ())))

    loop(count * (count + 1) // 2, body)


def unpack_kernel(scale, p_ref, o_ref):
    count = o_ref.shape[0] // SUB

    def body(t):
        i, j = corner(t, count)
        block = p_ref[tile(t), :] * scale
        o_ref[tile(j), tile(i)] = block.T
        o_ref[tile(i), tile(j)] = block

    loop(count * (count + 1) // 2, body)


VM = pl.BlockSpec(memory_space=pltpu.VMEM)
ANY = pl.BlockSpec(memory_space=pl.ANY)


def call(kernel, out_shape, vmem_args, any_args=(), scratch=(), flops=0):
    return pl.pallas_call(
        kernel,
        out_shape=jax.ShapeDtypeStruct(out_shape, F32),
        in_specs=[VM] * len(vmem_args) + [ANY] * len(any_args),
        out_specs=VM,
        scratch_shapes=list(scratch),
        compiler_params=pltpu.CompilerParams(vmem_limit_bytes=40 * 2**20),
        cost_estimate=pl.CostEstimate(
            flops=flops, bytes_accessed=4 * out_shape[0] * out_shape[1], transcendentals=0
        ),
    )(*vmem_args, *any_args)


def block_scratch(blocks, terms, n, wc):
    return [
        pltpu.VMEM((blocks, n, n), F32),
        pltpu.VMEM((max(terms, 1), n, wc), BF16),
        pltpu.VMEM((max(terms, 1), n, wc), BF16),
        pltpu.SemaphoreType.DMA((blocks,)),
    ]


def flat(blocks):
    return [piece for mine, other in blocks for piece in mine + other]


def routes(s, nb):
    if nb == 4:
        return {0: [[(0, 1)], [(0, 2), (1, 3)]], 1: [[(1, 2)], [(1, 3)]], 2: [[(2, 3)]]}[s]
    return [[(s, b)] for b in range(s + 1, nb)]


def local(psi, lower):
    nb, ng = lax.axis_size("band"), lax.axis_size("ga")
    nq = ng // 2
    n, w = psi.shape
    band, ga = lax.axis_index("band"), lax.axis_index("ga")
    chip, core = ga // 2, ga % 2
    helped = HELPED.get(nb, {})

    def shift(x, hops):
        pairs = [
            (b * ng + q * 2 + c, bb * ng + qq * 2 + cc)
            for (b, q, c), (bb, qq, cc) in hops
        ]
        return lax.ppermute(x, AXES, pairs)

    def swap(x):
        return shift(
            x, [((b, q, c), (b, q, 1 - c)) for b in range(nb) for q in range(nq) for c in range(2)]
        )

    def between(x, hops):
        return shift(
            x, [((a, q, c), (b, q, c)) for a, b in hops for q in range(nq) for c in range(2)]
        )

    rows = n // PIECES
    own = [lower[i * rows : (i + 1) * rows] for i in range(PIECES)]
    ready = call(invert_kernel, lower.shape, [lower], flops=2**28)
    ready = [ready[i * rows : (i + 1) * rows] for i in range(PIECES)]

    lines, source = [], []
    for d in range(nb):
        line = {b: b - d for b in range(d, nb)}
        data = list(ready if d == 0 else own)
        if d in helped:
            b, h = helped[d]
            k = line.pop(b)
            line[h] = k
            for i in range(PIECES):
                moved = shift(own[i], [((b, k, c), (h, k, c)) for c in range(2)])
                data[i] = jnp.where(band == h, moved, own[i])
        lines.append(line)
        source.append(data)

    def holder(line):
        at = jnp.full((), -1, jnp.int32)
        for b, k in line.items():
            at = jnp.where(band == b, k, at)
        return chip == at

    held = []
    for d in range(nb):
        held.append([jnp.where(holder(lines[d]), x, 0.0) for x in source[d]])
    sent = source
    bit = nq // 2
    first = True
    while bit:
        for d in range(nb):
            for i in range(PIECES):
                hops = []
                for b, k in lines[d].items():
                    for q in range(nq):
                        if (q ^ k) & (2 * bit - 1) == 0:
                            for c in range(2):
                                if d == 0 and c * (n // 2) >= (i + 1) * rows:
                                    continue
                                hops.append(((b, q, c), (b, q ^ bit, c)))
                got = shift(source[d][i] if first else held[d][i], hops)
                held[d][i] = held[d][i] + got
        first = False
        bit //= 2
    blocks = []
    for d in range(nb):
        blocks.append((held[d], [swap(x) for x in held[d]]))

    wc = w // CHUNKS
    psis = [psi[:, k * wc : (k + 1) * wc] for k in range(CHUNKS)]
    outs = []
    seen = [[] for _ in range(CHUNKS)]
    parts = [{} for _ in range(CHUNKS)]
    assist = {h: (d, b) for d, (b, h) in helped.items()}
    aided = {b: h for d, (b, h) in helped.items()}
    done = [jnp.zeros((n, wc), F32) for _ in range(CHUNKS)]
    for s in range(nb):
        for x in range(CHUNKS):
            partial = s in aided
            used = [k for k in range(s) if not (partial and k == aided[s])]
            need = [blocks[0]] + [blocks[s - k] for k in used]
            solved = call(
                functools.partial(solve_kernel, s, partial, PIECES),
                (n, wc),
                [psis[x]]
                + ([parts[x][s]] if partial else [])
                + [seen[x][k] for k in used],
                flat(need),
                block_scratch(len(need), len(used), n, wc),
                2 * n * n * wc * (2 * s + 1),
            )
            done[x] = jnp.where(band == s, solved, done[x])
            if s == nb - 1:
                continue
            total = jnp.where(band == s, solved, 0.0)
            for hops in routes(s, nb):
                give = total
                if s in assist and (s, assist[s][1]) in hops:
                    give = call(
                        functools.partial(term_kernel, s, PIECES),
                        (n, wc),
                        [total],
                        flat([blocks[assist[s][0]]]),
                        block_scratch(1, 1, n, wc),
                        4 * n * n * wc,
                    )
                    got = between(give, hops)
                    parts[x][assist[s][1]] = got
                else:
                    got = between(give, hops)
                total = total + got
            seen[x].append(total)
    full = jnp.concatenate(done, axis=1)

    count = n // SUB
    tri = count * (count + 1) // 2 * SUB
    packed = call(
        gram_kernel,
        (tri, SUB),
        [full],
        scratch=[pltpu.VMEM((n, w), BF16), pltpu.VMEM((n, w), BF16)],
        flops=3 * n * n * w,
    )
    half = tri // 2
    mine = lax.dynamic_slice_in_dim(packed, core * half, half, 0)
    give = lax.dynamic_slice_in_dim(packed, (1 - core) * half, half, 0)
    mine = mine + swap(give)
    part = half // nq
    away = lambda x, d: shift(
        x,
        [((b, q, c), (b, q ^ d, c)) for b in range(nb) for q in range(nq) for c in range(2)],
    )
    piece = lambda q: lax.dynamic_slice_in_dim(mine, q * part, part, 0)
    total = piece(chip)
    for d in range(1, nq):
        total = total + away(piece(chip ^ d), d)
    result = jnp.zeros((half, SUB), F32)
    result = lax.dynamic_update_slice_in_dim(result, total, chip * part, 0)
    for d in range(1, nq):
        result = lax.dynamic_update_slice_in_dim(result, away(total, d), (chip ^ d) * part, 0)
    theirs = swap(result)
    whole = jnp.zeros((tri, SUB), F32)
    whole = lax.dynamic_update_slice_in_dim(whole, result, core * half, 0)
    whole = lax.dynamic_update_slice_in_dim(whole, theirs, (1 - core) * half, 0)
    inter = call(
        functools.partial(unpack_kernel, 1.0 / (w * ng)), (n, n), [whole], flops=4 * n * n
    )
    return (full, inter)


def solution(mesh):
    return jax.shard_map(
        local,
        mesh=mesh,
        in_specs=(P("band", "ga"), P("band", "ga")),
        out_specs=(P("band", "ga"), P("band", None)),
        check_vma=False,
    )
```

```python
import functools
import jax
import jax.numpy as jnp
from jax import lax
from jax.experimental import pallas as pl
from jax.experimental.pallas import tpu as pltpu
from jax.sharding import PartitionSpec as P


AXES = ("band", "ga")
F32, BF16 = jnp.float32, jnp.bfloat16
PIECES = 2
CHUNKS = 2
SUB = 256


def split(x):
    hi = x.astype(BF16)
    return hi, (x - hi.astype(F32)).astype(BF16)


def mm(a, b, dims=(((1,), (0,)), ((), ()))):
    dot = functools.partial(lax.dot_general, dimension_numbers=dims, preferred_element_type=F32)
    return dot(a[0], b[0]) + (dot(a[0], b[1]) + dot(a[1], b[0]))


def tile(i):
    return pl.ds(pl.multiple_of(i * SUB, SUB), SUB)


def loop(count, body):
    lax.fori_loop(0, count, lambda i, _: (body(i), 0)[1], 0)


def invert_kernel(l_ref, *refs):
    outs, o_ref = refs[:-1], refs[-1]
    band, ga = lax.axis_index("band"), lax.axis_index("ga")
    n, wide = l_ref.shape
    o_ref[...] = l_ref[...]

    @pl.when(ga // 2 == band)
    def _():
        first = (ga % 2) * wide
        row = lax.broadcasted_iota(jnp.int32, (SUB, SUB), 0)
        col = lax.broadcasted_iota(jnp.int32, (SUB, SUB), 1)
        spots = [
            (pl.ds(pl.multiple_of(first + i * SUB, SUB), SUB), pl.ds(i * SUB, SUB))
            for i in range(wide // SUB)
        ]
        for at in spots:
            t = l_ref[at]
            d = jnp.where(row == col, t, 0.0)
            rd = 1.0 / jnp.sum(d, axis=1, keepdims=True)
            cd = 1.0 / jnp.sum(d, axis=0, keepdims=True)
            pair = (row == col + 1) & (row % 2 == 1)
            o_ref[at] = jnp.where(row == col, rd, jnp.where(pair, -t * rd * cd, 0.0))

        def level(k):
            r, c = lax.shift_right_logical(row, k), lax.shift_right_logical(col, k)
            mask = (r == c + 1) & (r % 2 == 1)
            xs = [o_ref[at] for at in spots]
            ys = [split(x) for x in xs]
            mid = [mm(split(jnp.where(mask, l_ref[at], 0.0)), y) for at, y in zip(spots, ys)]
            for at, x, y, v in zip(spots, xs, ys, mid):
                o_ref[at] = x - mm(y, split(v))

        loop(SUB.bit_length() - 2, lambda k: level(k + 1))

    rows = n // len(outs)
    for i, out in enumerate(outs):
        out[...] = o_ref[pl.ds(i * rows, rows), :]


def pick_kernel(take_own, own_ref, *refs):
    got, o_ref = refs[:-1], refs[-1]
    mine = take_own(lax.axis_index("band"), lax.axis_index("ga"))

    @pl.when(mine)
    def _():
        o_ref[...] = own_ref[...]

    @pl.when(jnp.logical_not(mine))
    def _():
        value = got[0][...]
        for ref in got[1:]:
            value = value + ref[...]
        o_ref[...] = value


def pick(take_own, own, *got):
    return call(functools.partial(pick_kernel, take_own), own.shape, [own, *got], flops=own.size)


def fetch(blocks, lbuf, sem, core):
    wide = lbuf.shape[2] // 2
    copies = []
    for d, (mine, other) in enumerate(blocks):
        for pieces, side in ((mine, core), (other, 1 - core)):
            row = 0
            for piece in pieces:
                to = lbuf.at[d, pl.ds(row, piece.shape[0]), pl.ds(pl.multiple_of(side * wide, wide), wide)]
                copies.append(pltpu.make_async_copy(piece, to, sem.at[d]))
                row += piece.shape[0]
    return copies


def unflatten(refs, pieces):
    it = iter(refs)
    blocks = []
    while len(blocks) * 2 * pieces < len(refs):
        blocks.append(([next(it) for _ in range(pieces)], [next(it) for _ in range(pieces)]))
    return blocks


def product_update(o_ref, lbuf, d, yh, yl, k):
    n = lbuf.shape[1]
    depth = min(2 * SUB, n)

    def body(t):
        i, j = t // (n // depth), t % (n // depth)
        cols = pl.ds(pl.multiple_of(j * depth, depth), depth)
        part = mm(split(lbuf[d, tile(i), cols]), (yh[k, cols, :], yl[k, cols, :]))
        o_ref[tile(i), :] = o_ref[tile(i), :] - part

    loop(n // SUB * (n // depth), body)


def band_kernel(s, final, pieces, given, *refs):
    r_ref, y_refs, refs = refs[0], refs[1 : 1 + given], refs[1 + given :]
    nblocks = given + (1 if final else 0)
    blocks = unflatten(refs[: nblocks * 2 * pieces], pieces)
    o_ref, lbuf, yh, yl, sem = refs[nblocks * 2 * pieces :]
    band, core = lax.axis_index("band"), lax.axis_index("ga") % 2
    n = lbuf.shape[1]

    @pl.when(band == s)
    def _():
        copies = fetch(blocks, lbuf, sem, core)
        for copy in copies:
            copy.start()
        o_ref[...] = r_ref[...]
        for k in range(given):

            def spread(i):
                yh[k, tile(i), :], yl[k, tile(i), :] = split(y_refs[k][tile(i), :])

            loop(n // SUB, spread)
        for copy in copies:
            copy.wait()
        if given:
            loop(given, lambda k: product_update(o_ref, lbuf, k, yh, yl, k))
        if not final:
            return

        def step(i):
            y = mm(split(lbuf[given, tile(i), tile(i)]), split(o_ref[tile(i), :]))
            o_ref[tile(i), :] = y
            y = split(y)

            def below(j, _):
                o_ref[tile(j), :] = o_ref[tile(j), :] - mm(split(lbuf[given, tile(j), tile(i)]), y)
                return 0

            lax.fori_loop(i + 1, n // SUB, below, 0)

        loop(n // SUB, step)


def corner(t, count):
    i = sum((t >= k * (k + 1) // 2).astype(jnp.int32) for k in range(1, count))
    return i, t - i * (i + 1) // 2


def gram_kernel(y_ref, o_ref, yh, yl):
    n = y_ref.shape[0]

    def spread(i):
        yh[tile(i), :], yl[tile(i), :] = split(y_ref[tile(i), :])

    loop(n // SUB, spread)
    count = n // SUB

    def body(t):
        i, j = corner(t, count)
        a, b = (yh[tile(i), :], yl[tile(i), :]), (yh[tile(j), :], yl[tile(j), :])
        o_ref[tile(t), :] = mm(a, b, (((1,), (1,)), ((), ())))

    loop(count * (count + 1) // 2, body)


def unpack_kernel(scale, p_ref, o_ref):
    count = o_ref.shape[0] // SUB

    def body(t):
        i, j = corner(t, count)
        block = p_ref[tile(t), :] * scale
        o_ref[tile(j), tile(i)] = block.T
        o_ref[tile(i), tile(j)] = block

    loop(count * (count + 1) // 2, body)


VM = pl.BlockSpec(memory_space=pltpu.VMEM)
ANY = pl.BlockSpec(memory_space=pl.ANY)


def call(kernel, out_shape, vmem_args, any_args=(), scratch=(), flops=0):
    return pl.pallas_call(
        kernel,
        out_shape=jax.ShapeDtypeStruct(out_shape, F32),
        in_specs=[VM] * len(vmem_args) + [ANY] * len(any_args),
        out_specs=VM,
        scratch_shapes=list(scratch),
        compiler_params=pltpu.CompilerParams(vmem_limit_bytes=40 * 2**20),
        cost_estimate=pl.CostEstimate(
            flops=flops, bytes_accessed=4 * out_shape[0] * out_shape[1], transcendentals=0
        ),
    )(*vmem_args, *any_args)


def block_scratch(blocks, terms, n, wc):
    return [
        pltpu.VMEM((blocks, n, n), F32),
        pltpu.VMEM((max(terms, 1), n, wc), BF16),
        pltpu.VMEM((max(terms, 1), n, wc), BF16),
        pltpu.SemaphoreType.DMA((blocks,)),
    ]


def flat(blocks):
    return [piece for mine, other in blocks for piece in mine + other]


def pick_band(a, own, other):
    return pick(lambda band, ga: band == a, own, other)


def routes(s, nb):
    if nb == 4:
        return {0: [[(0, 1)], [(0, 2), (1, 3)]], 1: [[(1, 2)], [(1, 3)]], 2: [[(2, 3)]]}[s]
    return [[(s, b)] for b in range(s + 1, nb)]


def stages(nq):
    return nq.bit_length() - 1


def local(psi, lower):
    nb, ng = lax.axis_size("band"), lax.axis_size("ga")
    nq = ng // 2
    n, w = psi.shape
    band, ga = lax.axis_index("band"), lax.axis_index("ga")
    chip, core = ga // 2, ga % 2

    def shift(x, hops):
        pairs = [
            (b * ng + q * 2 + c, bb * ng + qq * 2 + cc)
            for (b, q, c), (bb, qq, cc) in hops
        ]
        return lax.ppermute(x, AXES, pairs)

    def swap(x, bands):
        return shift(
            x, [((b, q, c), (b, q, 1 - c)) for b in bands for q in range(nq) for c in range(2)]
        )

    rows = n // PIECES
    cut = lambda x: [x[i * rows : (i + 1) * rows] for i in range(PIECES)]
    ready = pl.pallas_call(
        invert_kernel,
        out_shape=[jax.ShapeDtypeStruct((rows, lower.shape[1]), F32)] * PIECES,
        in_specs=[VM],
        out_specs=[VM] * PIECES,
        scratch_shapes=[pltpu.VMEM(lower.shape, F32)],
        cost_estimate=pl.CostEstimate(flops=2**28, bytes_accessed=2**22, transcendentals=0),
    )(lower)
    plain = lax.optimization_barrier(cut(lower))

    source = [ready] + [plain] * (nb - 1)
    got = [[[] for _ in range(PIECES)] for _ in range(nb)]

    def merged(d, i):
        if not got[d][i]:
            return source[d][i]
        return pick(lambda band, ga: ga // 2 == band - d, source[d][i], *got[d][i])

    for t in range(stages(nq)):
        bit = nq >> (t + 1)
        for d in range(nb):
            for i in range(PIECES):
                hops = []
                for b in range(d, nb):
                    for q in range(nq):
                        if (q ^ (b - d)) & (2 * bit - 1) == 0:
                            for c in range(2):
                                if d or c * (n // 2) < (i + 1) * rows:
                                    hops.append(((b, q, c), (b, q ^ bit, c)))
                got[d][i].append(shift(merged(d, i), hops))
    blocks = []
    for d in range(nb):
        mine = [merged(d, i) for i in range(PIECES)]
        other = [swap(x, range(d, nb)) for x in mine]
        blocks.append((mine, other))

    wc = w // CHUNKS
    seen = [{} for _ in range(CHUNKS)]
    done = [[] for _ in range(CHUNKS)]

    def apply(s, final, rhs, x, ks):
        need = [blocks[s - k] for k in ks] + ([blocks[0]] if final else [])
        return call(
            lambda *refs: band_kernel(s, final, PIECES, len(ks), *refs),
            (n, wc),
            [rhs] + [seen[x][k, s] for k in ks],
            flat(need),
            block_scratch(len(need), len(ks), n, wc),
            6 * n * n * wc * (len(ks) + 1),
        )

    for s in range(nb):
        for x in range(CHUNKS):
            rhs = psi[:, x * wc : (x + 1) * wc]
            if s > 1:
                rhs = apply(s, False, rhs, x, list(range(s - 1)))
            solved = apply(s, True, rhs, x, [s - 1] if s else [])
            done[x].append(solved)
            have = {s: solved}
            for hops in routes(s, nb) if s + 1 < nb else []:
                give = None
                for a, _ in hops:
                    give = have[a] if give is None else pick_band(a, have[a], give)
                took = shift(
                    give,
                    [((a, q, c), (b, q, c)) for a, b in hops for q in range(nq) for c in range(2)],
                )
                for _, b in hops:
                    have[b] = seen[x][s, b] = took
    parts = []
    for x in range(CHUNKS):
        value = done[x][0]
        for s in range(1, nb):
            value = jnp.where(band == s, done[x][s], value)
        parts.append(value)
    full = jnp.concatenate(parts, axis=1)

    count = n // SUB
    tri = count * (count + 1) // 2 * SUB
    packed = call(
        gram_kernel,
        (tri, SUB),
        [full],
        scratch=[pltpu.VMEM((n, w), BF16), pltpu.VMEM((n, w), BF16)],
        flops=3 * n * n * w,
    )
    half = tri // 2
    mine = lax.dynamic_slice_in_dim(packed, core * half, half, 0)
    give = lax.dynamic_slice_in_dim(packed, (1 - core) * half, half, 0)
    mine = mine + swap(give, range(nb))
    part = half // nq
    away = lambda x, d: shift(
        x, [((b, q, c), (b, q ^ d, c)) for b in range(nb) for q in range(nq) for c in range(2)]
    )
    piece = lambda q: lax.dynamic_slice_in_dim(mine, q * part, part, 0)
    total = piece(chip)
    for d in range(1, nq):
        total = total + away(piece(chip ^ d), d)
    result = jnp.zeros((half, SUB), F32)
    result = lax.dynamic_update_slice_in_dim(result, total, chip * part, 0)
    for d in range(1, nq):
        result = lax.dynamic_update_slice_in_dim(result, away(total, d), (chip ^ d) * part, 0)
    theirs = swap(result, range(nb))
    whole = jnp.zeros((tri, SUB), F32)
    whole = lax.dynamic_update_slice_in_dim(whole, result, core * half, 0)
    whole = lax.dynamic_update_slice_in_dim(whole, theirs, (1 - core) * half, 0)
    inter = call(
        functools.partial(unpack_kernel, 1.0 / (w * ng)), (n, n), [whole], flops=4 * n * n
    )
    return (full, inter)


def solution(mesh):
    return jax.shard_map(
        local,
        mesh=mesh,
        in_specs=(P("band", "ga"), P("band", "ga")),
        out_specs=(P("band", "ga"), P("band", None)),
        check_vma=False,
    )
```

```python
import functools
import jax
import jax.numpy as jnp
from jax import lax
from jax.experimental import pallas as pl
from jax.experimental.pallas import tpu as pltpu
from jax.sharding import PartitionSpec as P


AXES = ("band", "ga")
F32, BF16 = jnp.float32, jnp.bfloat16
PIECES = 2
CHUNKS = 2
SUB = 256


def split(x):
    hi = x.astype(BF16)
    return hi, (x - hi.astype(F32)).astype(BF16)


def mm(a, b, dims=(((1,), (0,)), ((), ()))):
    dot = functools.partial(lax.dot_general, dimension_numbers=dims, preferred_element_type=F32)
    return dot(a[0], b[0]) + (dot(a[0], b[1]) + dot(a[1], b[0]))


def tile(i):
    return pl.ds(pl.multiple_of(i * SUB, SUB), SUB)


def loop(count, body):
    lax.fori_loop(0, count, lambda i, _: (body(i), 0)[1], 0)


def invert_kernel(l_ref, *refs):
    outs, o_ref = refs[:-1], refs[-1]
    band, ga = lax.axis_index("band"), lax.axis_index("ga")
    n, wide = l_ref.shape
    o_ref[...] = l_ref[...]

    @pl.when(ga // 2 == band)
    def _():
        first = (ga % 2) * wide
        row = lax.broadcasted_iota(jnp.int32, (SUB, SUB), 0)
        col = lax.broadcasted_iota(jnp.int32, (SUB, SUB), 1)
        spots = [
            (pl.ds(pl.multiple_of(first + i * SUB, SUB), SUB), pl.ds(i * SUB, SUB))
            for i in range(wide // SUB)
        ]
        for at in spots:
            t = l_ref[at]
            d = jnp.where(row == col, t, 0.0)
            rd = 1.0 / jnp.sum(d, axis=1, keepdims=True)
            cd = 1.0 / jnp.sum(d, axis=0, keepdims=True)
            pair = (row == col + 1) & (row % 2 == 1)
            o_ref[at] = jnp.where(row == col, rd, jnp.where(pair, -t * rd * cd, 0.0))

        def level(k):
            r, c = lax.shift_right_logical(row, k), lax.shift_right_logical(col, k)
            mask = (r == c + 1) & (r % 2 == 1)
            xs = [o_ref[at] for at in spots]
            ys = [split(x) for x in xs]
            mid = [mm(split(jnp.where(mask, l_ref[at], 0.0)), y) for at, y in zip(spots, ys)]
            for at, x, y, v in zip(spots, xs, ys, mid):
                o_ref[at] = x - mm(y, split(v))

        loop(SUB.bit_length() - 2, lambda k: level(k + 1))

    rows = n // len(outs)
    for i, out in enumerate(outs):
        out[...] = o_ref[pl.ds(i * rows, rows), :]


def pick_kernel(take_own, own_ref, *refs):
    got, o_ref = refs[:-1], refs[-1]
    mine = take_own(lax.axis_index("band"), lax.axis_index("ga"))

    @pl.when(mine)
    def _():
        o_ref[...] = own_ref[...]

    @pl.when(jnp.logical_not(mine))
    def _():
        value = got[0][...]
        for ref in got[1:]:
            value = value + ref[...]
        o_ref[...] = value


def pick(take_own, own, *got):
    return call(functools.partial(pick_kernel, take_own), own.shape, [own, *got], flops=own.size)


def gather_kernel(take_own, pieces, *refs):
    own, got, o_ref = refs[:pieces], refs[pieces:-1], refs[-1]
    mine = take_own(lax.axis_index("band"), lax.axis_index("ga"))
    rows = own[0].shape[0]
    for i in range(pieces):
        at = pl.ds(i * rows, rows)

        @pl.when(mine)
        def _():
            o_ref[at, :] = own[i][...]

        @pl.when(jnp.logical_not(mine))
        def _():
            value = got[i][...]
            for ref in got[i + pieces :: pieces]:
                value = value + ref[...]
            o_ref[at, :] = value


def gathered(take_own, own, got):
    shape = (sum(x.shape[0] for x in own), own[0].shape[1])
    kernel = functools.partial(gather_kernel, take_own, len(own))
    stages = len(got[0])
    return call(kernel, shape, [*own, *(x[t] for t in range(stages) for x in got)], flops=2**20)


def fetch(blocks, lbuf, sem, core):
    wide = lbuf.shape[2] // 2
    copies = []
    for d, (mine, other) in enumerate(blocks):
        for pieces, side in ((mine, core), (other, 1 - core)):
            row = 0
            for piece in pieces:
                to = lbuf.at[d, pl.ds(row, piece.shape[0]), pl.ds(pl.multiple_of(side * wide, wide), wide)]
                copies.append(pltpu.make_async_copy(piece, to, sem.at[d]))
                row += piece.shape[0]
    return copies


def unflatten(refs, pieces):
    it = iter(refs)
    blocks = []
    while len(blocks) * 2 * pieces < len(refs):
        blocks.append(([next(it) for _ in range(pieces)], [next(it) for _ in range(pieces)]))
    return blocks


def product_update(o_ref, lbuf, d, yh, yl, k):
    n = lbuf.shape[1]
    depth = min(2 * SUB, n)

    def body(t):
        i, j = t // (n // depth), t % (n // depth)
        cols = pl.ds(pl.multiple_of(j * depth, depth), depth)
        part = mm(split(lbuf[d, tile(i), cols]), (yh[k, cols, :], yl[k, cols, :]))
        o_ref[tile(i), :] = o_ref[tile(i), :] - part

    loop(n // SUB * (n // depth), body)


def band_kernel(s, final, pieces, given, *refs):
    r_ref, y_refs, refs = refs[0], refs[1 : 1 + given], refs[1 + given :]
    nblocks = given + (1 if final else 0)
    blocks = unflatten(refs[: nblocks * 2 * pieces], pieces)
    o_ref, lbuf, yh, yl, sem = refs[nblocks * 2 * pieces :]
    band, core = lax.axis_index("band"), lax.axis_index("ga") % 2
    n = lbuf.shape[1]

    @pl.when(band == s)
    def _():
        copies = fetch(blocks, lbuf, sem, core)
        for copy in copies:
            copy.start()
        o_ref[...] = r_ref[...]
        for k in range(given):

            def spread(i):
                yh[k, tile(i), :], yl[k, tile(i), :] = split(y_refs[k][tile(i), :])

            loop(n // SUB, spread)
        for copy in copies:
            copy.wait()
        if given:
            loop(given, lambda k: product_update(o_ref, lbuf, k, yh, yl, k))
        if not final:
            return

        def step(i):
            y = mm(split(lbuf[given, tile(i), tile(i)]), split(o_ref[tile(i), :]))
            o_ref[tile(i), :] = y
            y = split(y)

            def below(j, _):
                o_ref[tile(j), :] = o_ref[tile(j), :] - mm(split(lbuf[given, tile(j), tile(i)]), y)
                return 0

            lax.fori_loop(i + 1, n // SUB, below, 0)

        loop(n // SUB, step)


def corner(t, count):
    i = sum((t >= k * (k + 1) // 2).astype(jnp.int32) for k in range(1, count))
    return i, t - i * (i + 1) // 2


def gram_kernel(y_ref, o_ref, yh, yl):
    n = y_ref.shape[0]

    def spread(i):
        yh[tile(i), :], yl[tile(i), :] = split(y_ref[tile(i), :])

    loop(n // SUB, spread)
    count = n // SUB

    def body(t):
        i, j = corner(t, count)
        a, b = (yh[tile(i), :], yl[tile(i), :]), (yh[tile(j), :], yl[tile(j), :])
        o_ref[tile(t), :] = mm(a, b, (((1,), (1,)), ((), ())))

    loop(count * (count + 1) // 2, body)


def unpack_kernel(scale, p_ref, o_ref):
    count = o_ref.shape[0] // SUB

    def body(t):
        i, j = corner(t, count)
        block = p_ref[tile(t), :] * scale
        o_ref[tile(j), tile(i)] = block.T
        o_ref[tile(i), tile(j)] = block

    loop(count * (count + 1) // 2, body)


VM = pl.BlockSpec(memory_space=pltpu.VMEM)
ANY = pl.BlockSpec(memory_space=pl.ANY)


def call(kernel, out_shape, vmem_args, any_args=(), scratch=(), flops=0):
    return pl.pallas_call(
        kernel,
        out_shape=jax.ShapeDtypeStruct(out_shape, F32),
        in_specs=[VM] * len(vmem_args) + [ANY] * len(any_args),
        out_specs=VM,
        scratch_shapes=list(scratch),
        compiler_params=pltpu.CompilerParams(vmem_limit_bytes=40 * 2**20),
        cost_estimate=pl.CostEstimate(
            flops=flops, bytes_accessed=4 * out_shape[0] * out_shape[1], transcendentals=0
        ),
    )(*vmem_args, *any_args)


def block_scratch(blocks, terms, n, wc):
    return [
        pltpu.VMEM((blocks, n, n), F32),
        pltpu.VMEM((max(terms, 1), n, wc), BF16),
        pltpu.VMEM((max(terms, 1), n, wc), BF16),
        pltpu.SemaphoreType.DMA((blocks,)),
    ]


def flat(blocks):
    return [piece for mine, other in blocks for piece in mine + other]


def routes(s, nb):
    if nb == 4:
        return {0: [[(0, 1)], [(0, 2)], [(2, 3)]], 1: [[(1, 2)], [(1, 3)]], 2: [[(2, 3)]]}[s]
    return [[(s, b)] for b in range(s + 1, nb)]


def tree(k, nq):
    if nq == 4:
        return {
            0: [[(0, 2)], [(0, 1), (2, 3)]],
            1: [[(1, 2)], [(1, 0), (2, 3)]],
            2: [[(2, 3)], [(2, 0), (3, 1)]],
            3: [[(3, 1)], [(3, 2), (1, 0)]],
        }[k]
    steps = []
    bit = nq // 2
    while bit:
        steps.append([(q, q ^ bit) for q in range(nq) if (q ^ k) & (2 * bit - 1) == 0])
        bit //= 2
    return steps


def stages(nq):
    return nq.bit_length() - 1


def local(psi, lower):
    nb, ng = lax.axis_size("band"), lax.axis_size("ga")
    nq = ng // 2
    n, w = psi.shape
    band, ga = lax.axis_index("band"), lax.axis_index("ga")
    chip, core = ga // 2, ga % 2

    def shift(x, hops):
        pairs = [
            (b * ng + q * 2 + c, bb * ng + qq * 2 + cc)
            for (b, q, c), (bb, qq, cc) in hops
        ]
        return lax.ppermute(x, AXES, pairs)

    def swap(x, bands):
        return shift(
            x, [((b, q, c), (b, q, 1 - c)) for b in bands for q in range(nq) for c in range(2)]
        )

    rows = n // PIECES
    cut = lambda x: [x[i * rows : (i + 1) * rows] for i in range(PIECES)]
    ready = pl.pallas_call(
        invert_kernel,
        out_shape=[jax.ShapeDtypeStruct((rows, lower.shape[1]), F32)] * PIECES,
        in_specs=[VM],
        out_specs=[VM] * PIECES,
        scratch_shapes=[pltpu.VMEM(lower.shape, F32)],
        cost_estimate=pl.CostEstimate(flops=2**28, bytes_accessed=2**22, transcendentals=0),
    )(lower)
    plain = lax.optimization_barrier(cut(lower))

    source = [ready] + [plain] * (nb - 1)
    got = [[[] for _ in range(PIECES)] for _ in range(nb)]

    def merged(d, i):
        if not got[d][i]:
            return source[d][i]
        return pick(lambda band, ga: ga // 2 == band - d, source[d][i], *got[d][i])

    for t in range(stages(nq)):
        for d in range(nb):
            for i in range(PIECES):
                hops = [
                    ((b, q, c), (b, to, c))
                    for b in range(d, nb)
                    for q, to in tree(b - d, nq)[t]
                    for c in range(2)
                    if d or c * (n // 2) < (i + 1) * rows
                ]
                got[d][i].append(shift(merged(d, i), hops))
    blocks = []
    for d in range(nb):
        mine = gathered(lambda band, ga: ga // 2 == band - d, source[d], got[d])
        blocks.append(([mine], [swap(mine, range(d, nb))]))

    wc = w // CHUNKS
    seen = [{} for _ in range(CHUNKS)]
    done = [[] for _ in range(CHUNKS)]

    def apply(s, final, rhs, x, ks):
        need = [blocks[s - k] for k in ks] + ([blocks[0]] if final else [])
        return call(
            lambda *refs: band_kernel(s, final, 1, len(ks), *refs),
            (n, wc),
            [rhs] + [seen[x][k, s] for k in ks],
            flat(need),
            block_scratch(len(need), len(ks), n, wc),
            6 * n * n * wc * (len(ks) + 1),
        )

    for s in range(nb):
        for x in range(CHUNKS):
            rhs = psi[:, x * wc : (x + 1) * wc]
            if s > 1:
                rhs = apply(s, False, rhs, x, list(range(s - 1)))
            solved = apply(s, True, rhs, x, [s - 1] if s else [])
            done[x].append(solved)
            have = {s: solved}
            for hops in routes(s, nb) if s + 1 < nb else []:
                give = have[hops[0][0]]
                took = shift(
                    give,
                    [((a, q, c), (b, q, c)) for a, b in hops for q in range(nq) for c in range(2)],
                )
                for _, b in hops:
                    have[b] = seen[x][s, b] = took
    parts = []
    for x in range(CHUNKS):
        value = done[x][0]
        for s in range(1, nb):
            value = jnp.where(band == s, done[x][s], value)
        parts.append(value)
    full = jnp.concatenate(parts, axis=1)

    count = n // SUB
    tri = count * (count + 1) // 2 * SUB
    packed = call(
        gram_kernel,
        (tri, SUB),
        [full],
        scratch=[pltpu.VMEM((n, w), BF16), pltpu.VMEM((n, w), BF16)],
        flops=3 * n * n * w,
    )
    half = tri // 2
    mine = lax.dynamic_slice_in_dim(packed, core * half, half, 0)
    give = lax.dynamic_slice_in_dim(packed, (1 - core) * half, half, 0)
    mine = mine + swap(give, range(nb))
    part = half // nq
    away = lambda x, d: shift(
        x, [((b, q, c), (b, q ^ d, c)) for b in range(nb) for q in range(nq) for c in range(2)]
    )
    piece = lambda q: lax.dynamic_slice_in_dim(mine, q * part, part, 0)
    total = piece(chip)
    for d in range(1, nq):
        total = total + away(piece(chip ^ d), d)
    result = jnp.zeros((half, SUB), F32)
    result = lax.dynamic_update_slice_in_dim(result, total, chip * part, 0)
    for d in range(1, nq):
        result = lax.dynamic_update_slice_in_dim(result, away(total, d), (chip ^ d) * part, 0)
    theirs = swap(result, range(nb))
    whole = jnp.zeros((tri, SUB), F32)
    whole = lax.dynamic_update_slice_in_dim(whole, result, core * half, 0)
    whole = lax.dynamic_update_slice_in_dim(whole, theirs, (1 - core) * half, 0)
    inter = call(
        functools.partial(unpack_kernel, 1.0 / (w * ng)), (n, n), [whole], flops=4 * n * n
    )
    return (full, inter)


def solution(mesh):
    return jax.shard_map(
        local,
        mesh=mesh,
        in_specs=(P("band", "ga"), P("band", "ga")),
        out_specs=(P("band", "ga"), P("band", None)),
        check_vma=False,
    )
```

```python
import functools
import jax
import jax.numpy as jnp
from jax import lax
from jax.experimental import pallas as pl
from jax.experimental.pallas import tpu as pltpu
from jax.sharding import PartitionSpec as P


AXES = ("band", "ga")
F32, BF16 = jnp.float32, jnp.bfloat16


def bounds(d, n):
    return (0, n // 2, 3 * n // 4, n) if d == 0 else (0, n // 2, n)


CHUNKS = 2
SUB = 256


def split(x):
    hi = x.astype(BF16)
    return hi, (x - hi.astype(F32)).astype(BF16)


def mm(a, b, dims=(((1,), (0,)), ((), ()))):
    dot = functools.partial(lax.dot_general, dimension_numbers=dims, preferred_element_type=F32)
    return dot(a[0], b[0]) + (dot(a[0], b[1]) + dot(a[1], b[0]))


def tile(i):
    return pl.ds(pl.multiple_of(i * SUB, SUB), SUB)


def loop(count, body):
    lax.fori_loop(0, count, lambda i, _: (body(i), 0)[1], 0)


def invert_kernel(l_ref, *refs):
    outs, o_ref = refs[:-1], refs[-1]
    band, ga = lax.axis_index("band"), lax.axis_index("ga")
    _, wide = l_ref.shape
    o_ref[...] = l_ref[...]

    @pl.when(ga // 2 == band)
    def _():
        first = (ga % 2) * wide
        row = lax.broadcasted_iota(jnp.int32, (SUB, SUB), 0)
        col = lax.broadcasted_iota(jnp.int32, (SUB, SUB), 1)
        spots = [
            (pl.ds(pl.multiple_of(first + i * SUB, SUB), SUB), pl.ds(i * SUB, SUB))
            for i in range(wide // SUB)
        ]
        for at in spots:
            t = l_ref[at]
            d = jnp.where(row == col, t, 0.0)
            rd = 1.0 / jnp.sum(d, axis=1, keepdims=True)
            cd = 1.0 / jnp.sum(d, axis=0, keepdims=True)
            pair = (row == col + 1) & (row % 2 == 1)
            o_ref[at] = jnp.where(row == col, rd, jnp.where(pair, -t * rd * cd, 0.0))

        def level(k):
            r, c = lax.shift_right_logical(row, k), lax.shift_right_logical(col, k)
            mask = (r == c + 1) & (r % 2 == 1)
            xs = [o_ref[at] for at in spots]
            ys = [split(x) for x in xs]
            mid = [mm(split(jnp.where(mask, l_ref[at], 0.0)), y) for at, y in zip(spots, ys)]
            for at, x, y, v in zip(spots, xs, ys, mid):
                o_ref[at] = x - mm(y, split(v))

        loop(SUB.bit_length() - 2, lambda k: level(k + 1))

    row = 0
    for out in outs:
        out[...] = o_ref[pl.ds(row, out.shape[0]), :]
        row += out.shape[0]


def pick_kernel(take_own, own_ref, *refs):
    got, o_ref = refs[:-1], refs[-1]
    mine = take_own(lax.axis_index("band"), lax.axis_index("ga"))

    @pl.when(mine)
    def _():
        o_ref[...] = own_ref[...]

    @pl.when(jnp.logical_not(mine))
    def _():
        value = got[0][...]
        for ref in got[1:]:
            value = value + ref[...]
        o_ref[...] = value


def pick(take_own, own, *got):
    return call(functools.partial(pick_kernel, take_own), own.shape, [own, *got], flops=own.size)


def gather_kernel(take_own, pieces, got, *refs):
    own, got, o_ref = refs[:pieces], refs[pieces : pieces + got], refs[-1]
    mine = take_own(lax.axis_index("band"), lax.axis_index("ga"))
    row = 0
    for i in range(pieces):
        at = pl.ds(row, own[i].shape[0])
        row += own[i].shape[0]

        @pl.when(mine)
        def _():
            o_ref[at, :] = own[i][...]

        @pl.when(jnp.logical_not(mine))
        def _():
            value = got[i][...]
            for ref in got[i + pieces :: pieces]:
                value = value + ref[...]
            o_ref[at, :] = value


def gathered(take_own, own, got, after):
    shape = (sum(x.shape[0] for x in own), own[0].shape[1])
    flat = [x[t] for t in range(len(got[0])) for x in got]
    kernel = functools.partial(gather_kernel, take_own, len(own), len(flat))
    return call(kernel, shape, [*own, *flat], after, flops=2**20)


def fetch(blocks, lbuf, sem, core):
    wide = lbuf.shape[2] // 2
    copies = []
    for d, (mine, other) in enumerate(blocks):
        for pieces, side in ((mine, core), (other, 1 - core)):
            row = 0
            for piece in pieces:
                to = lbuf.at[d, pl.ds(row, piece.shape[0]), pl.ds(pl.multiple_of(side * wide, wide), wide)]
                copies.append(pltpu.make_async_copy(piece, to, sem.at[d]))
                row += piece.shape[0]
    return copies


def unflatten(refs, pieces):
    it = iter(refs)
    blocks = []
    while len(blocks) * 2 * pieces < len(refs):
        blocks.append(([next(it) for _ in range(pieces)], [next(it) for _ in range(pieces)]))
    return blocks


def product_update(o_ref, lbuf, d, yh, yl, k):
    n = lbuf.shape[1]
    depth = min(2 * SUB, n)

    def body(t):
        i, j = t // (n // depth), t % (n // depth)
        cols = pl.ds(pl.multiple_of(j * depth, depth), depth)
        part = mm(split(lbuf[d, tile(i), cols]), (yh[k, cols, :], yl[k, cols, :]))
        o_ref[tile(i), :] = o_ref[tile(i), :] - part

    loop(n // SUB * (n // depth), body)


def band_kernel(s, final, pieces, given, *refs):
    r_ref, y_refs, refs = refs[0], refs[1 : 1 + given], refs[1 + given :]
    nblocks = given + (1 if final else 0)
    blocks = unflatten(refs[: nblocks * 2 * pieces], pieces)
    o_ref, lbuf, yh, yl, sem = refs[nblocks * 2 * pieces :]
    band, core = lax.axis_index("band"), lax.axis_index("ga") % 2
    n = lbuf.shape[1]

    @pl.when(band == s)
    def _():
        copies = fetch(blocks, lbuf, sem, core)
        for copy in copies:
            copy.start()
        o_ref[...] = r_ref[...]
        for k in range(given):

            def spread(i):
                yh[k, tile(i), :], yl[k, tile(i), :] = split(y_refs[k][tile(i), :])

            loop(n // SUB, spread)
        for copy in copies:
            copy.wait()
        if given:
            loop(given, lambda k: product_update(o_ref, lbuf, k, yh, yl, k))
        if not final:
            return

        def step(i):
            y = mm(split(lbuf[given, tile(i), tile(i)]), split(o_ref[tile(i), :]))
            o_ref[tile(i), :] = y
            y = split(y)

            def below(j, _):
                o_ref[tile(j), :] = o_ref[tile(j), :] - mm(split(lbuf[given, tile(j), tile(i)]), y)
                return 0

            lax.fori_loop(i + 1, n // SUB, below, 0)

        loop(n // SUB, step)


def corner(t, count):
    i = sum((t >= k * (k + 1) // 2).astype(jnp.int32) for k in range(1, count))
    return i, t - i * (i + 1) // 2


def gram_kernel(y_ref, o_ref, yh, yl):
    n = y_ref.shape[0]

    def spread(i):
        yh[tile(i), :], yl[tile(i), :] = split(y_ref[tile(i), :])

    loop(n // SUB, spread)
    count = n // SUB

    def body(t):
        i, j = corner(t, count)
        a, b = (yh[tile(i), :], yl[tile(i), :]), (yh[tile(j), :], yl[tile(j), :])
        o_ref[tile(t), :] = mm(a, b, (((1,), (1,)), ((), ())))

    loop(count * (count + 1) // 2, body)


def unpack_kernel(scale, p_ref, o_ref):
    count = o_ref.shape[0] // SUB

    def body(t):
        i, j = corner(t, count)
        block = p_ref[tile(t), :] * scale
        o_ref[tile(j), tile(i)] = block.T
        o_ref[tile(i), tile(j)] = block

    loop(count * (count + 1) // 2, body)


VM = pl.BlockSpec(memory_space=pltpu.VMEM)
ANY = pl.BlockSpec(memory_space=pl.ANY)


def call(kernel, out_shape, vmem_args, any_args=(), scratch=(), flops=0):
    return pl.pallas_call(
        kernel,
        out_shape=jax.ShapeDtypeStruct(out_shape, F32),
        in_specs=[VM] * len(vmem_args) + [ANY] * len(any_args),
        out_specs=VM,
        scratch_shapes=list(scratch),
        compiler_params=pltpu.CompilerParams(vmem_limit_bytes=40 * 2**20),
        cost_estimate=pl.CostEstimate(
            flops=flops, bytes_accessed=4 * out_shape[0] * out_shape[1], transcendentals=0
        ),
    )(*vmem_args, *any_args)


def block_scratch(blocks, terms, n, wc):
    return [
        pltpu.VMEM((blocks, n, n), F32),
        pltpu.VMEM((max(terms, 1), n, wc), BF16),
        pltpu.VMEM((max(terms, 1), n, wc), BF16),
        pltpu.SemaphoreType.DMA((blocks,)),
    ]


def flat(blocks):
    return [piece for mine, other in blocks for piece in mine + other]


def routes(s, nb):
    if nb == 4:
        return {0: [[(0, 1)], [(0, 2)], [(2, 3)]], 1: [[(1, 2)], [(1, 3)]], 2: [[(2, 3)]]}[s]
    return [[(s, b)] for b in range(s + 1, nb)]


def tree(b, k, nq):
    if nq == 4:
        far = (b, k) in ((2, 0), (3, 0), (1, 0))
        return {
            0: [[(0, 2)], [(0, 1), (2, 3)]] if far else [[(0, 3)], [(0, 1), (3, 2)]],
            1: [[(1, 2)], [(1, 0), (2, 3)]] if b == 3 else [[(1, 3)], [(1, 0), (3, 2)]],
            2: [[(2, 3)], [(2, 0), (3, 1)]],
            3: [[(3, 1)], [(3, 2), (1, 0)]],
        }[k]
    steps = []
    bit = nq // 2
    while bit:
        steps.append([(q, q ^ bit) for q in range(nq) if (q ^ k) & (2 * bit - 1) == 0])
        bit //= 2
    return steps


def stages(nq):
    return nq.bit_length() - 1


def local(psi, lower):
    nb, ng = lax.axis_size("band"), lax.axis_size("ga")
    nq = ng // 2
    n, w = psi.shape
    band, ga = lax.axis_index("band"), lax.axis_index("ga")
    chip, core = ga // 2, ga % 2

    def shift(x, hops):
        pairs = [
            (b * ng + q * 2 + c, bb * ng + qq * 2 + cc)
            for (b, q, c), (bb, qq, cc) in hops
        ]
        return lax.ppermute(x, AXES, pairs)

    def swap(x, bands):
        return shift(
            x, [((b, q, c), (b, q, 1 - c)) for b in bands for q in range(nq) for c in range(2)]
        )

    ready = pl.pallas_call(
        invert_kernel,
        out_shape=[
            jax.ShapeDtypeStruct((z - a, lower.shape[1]), F32)
            for a, z in zip(bounds(0, n), bounds(0, n)[1:])
        ],
        in_specs=[VM],
        out_specs=[VM] * (len(bounds(0, n)) - 1),
        scratch_shapes=[pltpu.VMEM(lower.shape, F32)],
        cost_estimate=pl.CostEstimate(flops=2**28, bytes_accessed=2**22, transcendentals=0),
    )(lower)
    limits = bounds(1, n)
    plain = lax.optimization_barrier([lower[a:z] for a, z in zip(limits, limits[1:])])

    source = [ready] + [plain] * (nb - 1)
    got = [[[] for _ in source[d]] for d in range(nb)]

    def merged(d, i):
        if not got[d][i]:
            return source[d][i]
        return pick(lambda band, ga: ga // 2 == band - d, source[d][i], *got[d][i])

    for t in range(stages(nq)):
        for d in range(nb):
            for i in range(len(source[d])):
                hops = [
                    ((b, q, c), (b, to, c))
                    for b in range(d, nb)
                    for q, to in tree(b, b - d, nq)[t]
                    for c in range(2)
                    if d or c * (n // 2) < bounds(0, n)[i + 1]
                ]
                got[d][i].append(shift(merged(d, i), hops))
    blocks = []

    def land(d, after):
        own = lambda band, ga: ga // 2 == band - d
        mine = gathered(own, source[d], got[d], after)
        blocks.append(([mine], [swap(mine, range(nb))]))

    land(0, [])
    wc = w // CHUNKS
    seen = [{} for _ in range(CHUNKS)]
    done = [[] for _ in range(CHUNKS)]

    def apply(s, final, rhs, x, ks):
        need = [blocks[s - k] for k in ks] + ([blocks[0]] if final else [])
        return call(
            lambda *refs: band_kernel(s, final, 1, len(ks), *refs),
            (n, wc),
            [rhs] + [seen[x][k, s] for k in ks],
            flat(need),
            block_scratch(len(need), len(ks), n, wc),
            6 * n * n * wc * (len(ks) + 1),
        )

    for s in range(nb):
        if s:
            land(s, [done[-1][s - 1]])
        for x in range(CHUNKS):
            rhs = psi[:, x * wc : (x + 1) * wc]
            if s > 1:
                rhs = apply(s, False, rhs, x, list(range(s - 1)))
            solved = apply(s, True, rhs, x, [s - 1] if s else [])
            done[x].append(solved)
            have = {s: solved}
            for hops in routes(s, nb) if s + 1 < nb else []:
                give = have[hops[0][0]]
                took = shift(
                    give,
                    [((a, q, c), (b, q, c)) for a, b in hops for q in range(nq) for c in range(2)],
                )
                for _, b in hops:
                    have[b] = seen[x][s, b] = took
    parts = []
    for x in range(CHUNKS):
        value = done[x][0]
        for s in range(1, nb):
            value = jnp.where(band == s, done[x][s], value)
        parts.append(value)
    full = jnp.concatenate(parts, axis=1)

    count = n // SUB
    tri = count * (count + 1) // 2 * SUB
    packed = call(
        gram_kernel,
        (tri, SUB),
        [full],
        scratch=[pltpu.VMEM((n, w), BF16), pltpu.VMEM((n, w), BF16)],
        flops=3 * n * n * w,
    )
    half = tri // 2
    mine = lax.dynamic_slice_in_dim(packed, core * half, half, 0)
    give = lax.dynamic_slice_in_dim(packed, (1 - core) * half, half, 0)
    mine = mine + swap(give, range(nb))
    part = half // nq
    away = lambda x, d: shift(
        x, [((b, q, c), (b, q ^ d, c)) for b in range(nb) for q in range(nq) for c in range(2)]
    )
    piece = lambda q: lax.dynamic_slice_in_dim(mine, q * part, part, 0)
    total = piece(chip)
    for d in range(1, nq):
        total = total + away(piece(chip ^ d), d)
    result = jnp.zeros((half, SUB), F32)
    result = lax.dynamic_update_slice_in_dim(result, total, chip * part, 0)
    for d in range(1, nq):
        result = lax.dynamic_update_slice_in_dim(result, away(total, d), (chip ^ d) * part, 0)
    theirs = swap(result, range(nb))
    whole = jnp.zeros((tri, SUB), F32)
    whole = lax.dynamic_update_slice_in_dim(whole, result, core * half, 0)
    whole = lax.dynamic_update_slice_in_dim(whole, theirs, (1 - core) * half, 0)
    inter = call(
        functools.partial(unpack_kernel, 1.0 / (w * ng)), (n, n), [whole], flops=4 * n * n
    )
    return (full, inter)


def solution(mesh):
    return jax.shard_map(
        local,
        mesh=mesh,
        in_specs=(P("band", "ga"), P("band", "ga")),
        out_specs=(P("band", "ga"), P("band", None)),
        check_vma=False,
    )
```

```python
import functools
import jax
import jax.numpy as jnp
from jax import lax
from jax.experimental import pallas as pl
from jax.experimental.pallas import tpu as pltpu
from jax.sharding import PartitionSpec as P


AXES = ("band", "ga")
F32, BF16 = jnp.float32, jnp.bfloat16


def bounds(d, n):
    return (0, n // 2, 3 * n // 4, n) if d == "first" else (0, n // 2, n)


CHUNKS = 2
SUB = 256


def split(x):
    hi = x.astype(BF16)
    return hi, (x - hi.astype(F32)).astype(BF16)


def mm(a, b, dims=(((1,), (0,)), ((), ()))):
    dot = functools.partial(lax.dot_general, dimension_numbers=dims, preferred_element_type=F32)
    return dot(a[0], b[0]) + (dot(a[0], b[1]) + dot(a[1], b[0]))


def tile(i):
    return pl.ds(pl.multiple_of(i * SUB, SUB), SUB)


def loop(count, body):
    lax.fori_loop(0, count, lambda i, _: (body(i), 0)[1], 0)


def invert_kernel(l_ref, *refs):
    outs, o_ref = refs[:-1], refs[-1]
    band, ga = lax.axis_index("band"), lax.axis_index("ga")
    _, wide = l_ref.shape
    o_ref[...] = l_ref[...]

    @pl.when(ga // 2 == band)
    def _():
        first = (ga % 2) * wide
        row = lax.broadcasted_iota(jnp.int32, (SUB, SUB), 0)
        col = lax.broadcasted_iota(jnp.int32, (SUB, SUB), 1)
        spots = [
            (pl.ds(pl.multiple_of(first + i * SUB, SUB), SUB), pl.ds(i * SUB, SUB))
            for i in range(wide // SUB)
        ]
        for at in spots:
            t = l_ref[at]
            d = jnp.where(row == col, t, 0.0)
            rd = 1.0 / jnp.sum(d, axis=1, keepdims=True)
            cd = 1.0 / jnp.sum(d, axis=0, keepdims=True)
            pair = (row == col + 1) & (row % 2 == 1)
            o_ref[at] = jnp.where(row == col, rd, jnp.where(pair, -t * rd * cd, 0.0))

        def level(k):
            r, c = lax.shift_right_logical(row, k), lax.shift_right_logical(col, k)
            mask = (r == c + 1) & (r % 2 == 1)
            xs = [o_ref[at] for at in spots]
            ys = [split(x) for x in xs]
            mid = [mm(split(jnp.where(mask, l_ref[at], 0.0)), y) for at, y in zip(spots, ys)]
            for at, x, y, v in zip(spots, xs, ys, mid):
                o_ref[at] = x - mm(y, split(v))

        loop(SUB.bit_length() - 2, lambda k: level(k + 1))

    row = 0
    for out in outs:
        out[...] = o_ref[pl.ds(row, out.shape[0]), :]
        row += out.shape[0]


def choose_kernel(rules, pieces, *refs):
    o_ref = refs[-1]
    chip, band = lax.axis_index("ga") // 2, lax.axis_index("band")
    for u, rule in enumerate(rules):

        @pl.when(rule(band, chip))
        def _():
            row = 0
            for ref in refs[u * pieces : (u + 1) * pieces]:
                o_ref[pl.ds(row, ref.shape[0]), :] = ref[...]
                row += ref.shape[0]


def choose(rules, sources, after=()):
    pieces = len(sources[0])
    shape = (sum(x.shape[0] for x in sources[0]), sources[0][0].shape[1])
    given = [x for source in sources for x in source]

    def kernel(*refs):
        choose_kernel(rules, pieces, *refs[: len(given)], refs[-1])

    return call(kernel, shape, given, after, flops=2**20)


def taken(ks, stage, bit, nq):
    def rule(band, chip):
        found = False
        for k in ks:
            x = chip ^ (band - k)
            hit = x == 0 if stage < 0 else (x & -x) == (nq >> (stage + 1))
            if bit:
                hit = hit & ((x & (2 * bit - 1)) == 0)
            found = hit if found is False else found | hit
        return found

    return rule


def fetch(blocks, lbuf, sem, core):
    wide = lbuf.shape[2] // 2
    copies = []
    for d, (mine, other) in enumerate(blocks):
        for pieces, side in ((mine, core), (other, 1 - core)):
            row = 0
            for piece in pieces:
                to = lbuf.at[d, pl.ds(row, piece.shape[0]), pl.ds(pl.multiple_of(side * wide, wide), wide)]
                copies.append(pltpu.make_async_copy(piece, to, sem.at[d]))
                row += piece.shape[0]
    return copies


def unflatten(refs, pieces):
    it = iter(refs)
    blocks = []
    while len(blocks) * 2 * pieces < len(refs):
        blocks.append(([next(it) for _ in range(pieces)], [next(it) for _ in range(pieces)]))
    return blocks


def product_update(o_ref, lbuf, d, yh, yl, k):
    n = lbuf.shape[1]
    depth = min(2 * SUB, n)

    def body(t):
        i, j = t // (n // depth), t % (n // depth)
        cols = pl.ds(pl.multiple_of(j * depth, depth), depth)
        part = mm(split(lbuf[d, tile(i), cols]), (yh[k, cols, :], yl[k, cols, :]))
        o_ref[tile(i), :] = o_ref[tile(i), :] - part

    loop(n // SUB * (n // depth), body)


def band_kernel(s, final, pieces, given, after, *refs):
    r_ref, y_refs, refs = refs[0], refs[1 : 1 + given], refs[1 + given :]
    nblocks = given + (1 if final else 0)
    blocks = unflatten(refs[: nblocks * 2 * pieces], pieces)
    o_ref, lbuf, yh, yl, sem = refs[nblocks * 2 * pieces + after :]
    band, core = lax.axis_index("band"), lax.axis_index("ga") % 2
    n = lbuf.shape[1]

    @pl.when(band == s)
    def _():
        copies = fetch(blocks, lbuf, sem, core)
        for copy in copies:
            copy.start()
        o_ref[...] = r_ref[...]
        for k in range(given):

            def spread(i):
                yh[k, tile(i), :], yl[k, tile(i), :] = split(y_refs[k][tile(i), :])

            loop(n // SUB, spread)
        for copy in copies:
            copy.wait()
        if given:
            loop(given, lambda k: product_update(o_ref, lbuf, k, yh, yl, k))
        if not final:
            return

        def step(i):
            y = mm(split(lbuf[given, tile(i), tile(i)]), split(o_ref[tile(i), :]))
            o_ref[tile(i), :] = y
            y = split(y)

            def below(j, _):
                o_ref[tile(j), :] = o_ref[tile(j), :] - mm(split(lbuf[given, tile(j), tile(i)]), y)
                return 0

            lax.fori_loop(i + 1, n // SUB, below, 0)

        loop(n // SUB, step)


def corner(t, count):
    i = sum((t >= k * (k + 1) // 2).astype(jnp.int32) for k in range(1, count))
    return i, t - i * (i + 1) // 2


def gram_kernel(y_ref, o_ref, yh, yl):
    n = y_ref.shape[0]

    def spread(i):
        yh[tile(i), :], yl[tile(i), :] = split(y_ref[tile(i), :])

    loop(n // SUB, spread)
    count = n // SUB

    def body(t):
        i, j = corner(t, count)
        a, b = (yh[tile(i), :], yl[tile(i), :]), (yh[tile(j), :], yl[tile(j), :])
        o_ref[tile(t), :] = mm(a, b, (((1,), (1,)), ((), ())))

    loop(count * (count + 1) // 2, body)


def unpack_kernel(scale, p_ref, o_ref):
    count = o_ref.shape[0] // SUB

    def body(t):
        i, j = corner(t, count)
        block = p_ref[tile(t), :] * scale
        o_ref[tile(j), tile(i)] = block.T
        o_ref[tile(i), tile(j)] = block

    loop(count * (count + 1) // 2, body)


VM = pl.BlockSpec(memory_space=pltpu.VMEM)
ANY = pl.BlockSpec(memory_space=pl.ANY)


def call(kernel, out_shape, vmem_args, any_args=(), scratch=(), flops=0):
    return pl.pallas_call(
        kernel,
        out_shape=jax.ShapeDtypeStruct(out_shape, F32),
        in_specs=[VM] * len(vmem_args) + [ANY] * len(any_args),
        out_specs=VM,
        scratch_shapes=list(scratch),
        compiler_params=pltpu.CompilerParams(vmem_limit_bytes=40 * 2**20),
        cost_estimate=pl.CostEstimate(
            flops=flops, bytes_accessed=4 * out_shape[0] * out_shape[1], transcendentals=0
        ),
    )(*vmem_args, *any_args)


def block_scratch(blocks, terms, n, wc):
    return [
        pltpu.VMEM((blocks, n, n), F32),
        pltpu.VMEM((max(terms, 1), n, wc), BF16),
        pltpu.VMEM((max(terms, 1), n, wc), BF16),
        pltpu.SemaphoreType.DMA((blocks,)),
    ]


def flat(blocks):
    return [piece for mine, other in blocks for piece in mine + other]


def routes(s, nb):
    if nb == 4:
        return {0: [[(0, 1)], [(0, 2)], [(2, 3)]], 1: [[(1, 2)], [(1, 3)]], 2: [[(2, 3)]]}[s]
    return [[(s, b)] for b in range(s + 1, nb)]


def stages(nq):
    return nq.bit_length() - 1


def local(psi, lower):
    nb, ng = lax.axis_size("band"), lax.axis_size("ga")
    nq = ng // 2
    n, w = psi.shape
    band, ga = lax.axis_index("band"), lax.axis_index("ga")
    chip, core = ga // 2, ga % 2

    def shift(x, hops):
        pairs = [
            (b * ng + q * 2 + c, bb * ng + qq * 2 + cc)
            for (b, q, c), (bb, qq, cc) in hops
        ]
        return lax.ppermute(x, AXES, pairs)

    def swap(x, bands):
        return shift(
            x, [((b, q, c), (b, q, 1 - c)) for b in bands for q in range(nq) for c in range(2)]
        )

    ready = pl.pallas_call(
        invert_kernel,
        out_shape=[
            jax.ShapeDtypeStruct((z - a, lower.shape[1]), F32)
            for a, z in zip(bounds("first", n), bounds("first", n)[1:])
        ],
        in_specs=[VM],
        out_specs=[VM] * (len(bounds("first", n)) - 1),
        scratch_shapes=[pltpu.VMEM(lower.shape, F32)],
        cost_estimate=pl.CostEstimate(flops=2**28, bytes_accessed=2**22, transcendentals=0),
    )(lower)

    sets = {"first": (range(1), (0,)), "near": (range(1, nb), (0, 1))}
    sets.update({d: (range(d, nb), (d,)) for d in range(2, nb)})
    limits = bounds("near", n)
    plain = lax.optimization_barrier([lower[a:z] for a, z in zip(limits, limits[1:])])
    source = {d: plain for d in sets}
    source["first"] = ready
    source["near"] = [ready[0], choose([lambda band, chip: band >= 0], [ready[1:]])]
    got = {d: [[] for _ in source[d]] for d in sets}

    for t in range(stages(nq)):
        bit = nq >> (t + 1)
        for d, (bands, ks) in sets.items():
            for i in range(len(source[d])):
                hops = [
                    ((b, q, c), (b, q ^ bit, c))
                    for b in bands
                    for k in ks
                    for q in range(nq)
                    for c in range(2)
                    if (q ^ (b - k)) & (2 * bit - 1) == 0
                    and (k or c * (n // 2) < bounds(d, n)[i + 1])
                ]
                give = source[d][i]
                if t:
                    rules = [taken(ks, u, bit, nq) for u in range(-1, t)]
                    give = choose(rules, [[give]] + [[x] for x in got[d][i]])
                got[d][i].append(shift(give, hops))
    blocks = {}

    def land(name, d, k, after):
        rules = [taken((k,), u, 0, nq) for u in range(-1, stages(nq))]
        arrived = [[x[u] for x in got[d]] for u in range(stages(nq))]
        mine = choose(rules, [source[d]] + arrived, after)
        blocks[name] = ([mine], [swap(mine, range(nb))])

    land("first", "first", 0, [])
    wc = w // CHUNKS
    seen = [{} for _ in range(CHUNKS)]
    done = [[] for _ in range(CHUNKS)]

    def apply(s, final, rhs, x, ks, after):
        need = [blocks[s - k] for k in ks] + ([blocks["rest" if s else "first"]] if final else [])
        return call(
            lambda *refs: band_kernel(s, final, 1, len(ks), len(after), *refs),
            (n, wc),
            [rhs] + [seen[x][k, s] for k in ks],
            flat(need) + after,
            block_scratch(len(need), len(ks), n, wc),
            6 * n * n * wc * (len(ks) + 1),
        )

    for s in range(nb):
        if s:
            land(s, "near" if s == 1 else s, s, [done[-1][s - 1]])
        if s == 1:
            land("rest", "near", 0, [done[-1][0]])
        early = [psi[:, x * wc : (x + 1) * wc] for x in range(CHUNKS)]
        if s > 1:
            early = [apply(s, False, rhs, x, list(range(s - 1)), []) for x, rhs in enumerate(early)]
        for x in range(CHUNKS):
            solved = apply(s, True, early[x], x, [s - 1] if s else [], early if s == nb - 1 > 1 else [])
            done[x].append(solved)
            have = {s: solved}
            for hops in routes(s, nb) if s + 1 < nb else []:
                give = have[hops[0][0]]
                took = shift(
                    give,
                    [((a, q, c), (b, q, c)) for a, b in hops for q in range(nq) for c in range(2)],
                )
                for _, b in hops:
                    have[b] = seen[x][s, b] = took
    parts = []
    for x in range(CHUNKS):
        value = done[x][0]
        for s in range(1, nb):
            value = jnp.where(band == s, done[x][s], value)
        parts.append(value)
    full = jnp.concatenate(parts, axis=1)

    count = n // SUB
    tri = count * (count + 1) // 2 * SUB
    packed = call(
        gram_kernel,
        (tri, SUB),
        [full],
        scratch=[pltpu.VMEM((n, w), BF16), pltpu.VMEM((n, w), BF16)],
        flops=3 * n * n * w,
    )
    half = tri // 2
    mine = lax.dynamic_slice_in_dim(packed, core * half, half, 0)
    give = lax.dynamic_slice_in_dim(packed, (1 - core) * half, half, 0)
    mine = mine + swap(give, range(nb))
    part = half // nq
    away = lambda x, d: shift(
        x, [((b, q, c), (b, q ^ d, c)) for b in range(nb) for q in range(nq) for c in range(2)]
    )
    piece = lambda q: lax.dynamic_slice_in_dim(mine, q * part, part, 0)
    total = piece(chip)
    for d in range(1, nq):
        total = total + away(piece(chip ^ d), d)
    result = jnp.zeros((half, SUB), F32)
    result = lax.dynamic_update_slice_in_dim(result, total, chip * part, 0)
    for d in range(1, nq):
        result = lax.dynamic_update_slice_in_dim(result, away(total, d), (chip ^ d) * part, 0)
    theirs = swap(result, range(nb))
    whole = jnp.zeros((tri, SUB), F32)
    whole = lax.dynamic_update_slice_in_dim(whole, result, core * half, 0)
    whole = lax.dynamic_update_slice_in_dim(whole, theirs, (1 - core) * half, 0)
    inter = call(
        functools.partial(unpack_kernel, 1.0 / (w * ng)), (n, n), [whole], flops=4 * n * n
    )
    return (full, inter)


def solution(mesh):
    return jax.shard_map(
        local,
        mesh=mesh,
        in_specs=(P("band", "ga"), P("band", "ga")),
        out_specs=(P("band", "ga"), P("band", None)),
        check_vma=False,
    )
```
